128 devices in a mesh: lat: 16 (over x, z), lon: 8 (over y, core).
Axes of the slice: x: 4, y: 4, z: 4, core: 2. Of those that a mesh axis runs over, the one named last changes fastest.
Arguments:
- increment: bfloat16 [32, 16, 144, 128], P('lat', 'lon'), may hold values from -6 to 6
- cotangent: bfloat16 [16, 8, 40, 144, 128], P('lat', 'lon'), may hold values from -6 to 6
- weights: bfloat16 [16, 8, 40, 16, 128, 128], P('lat', 'lon'), may hold values from -0.1875 to 0.1875
- source_ids: int32 [16, 8, 40, 16], P('lat', 'lon'), may hold values from 0 to 511, as said below
- counts: int32 [16, 8, 40], P('lat', 'lon'), may hold values from 0 to 16, as said below
Outputs:
- ocean: bfloat16 [16, 8, 40, 144, 128], P('lat', 'lon')
- atmos_adjoint: bfloat16 [32, 16, 144, 128], P('lat', 'lon')
The draws below stay inside these ranges and needn't reach their ends.
Inputs may be any that keep to these rules, and one draw needn't show every extreme that they name: source_ids[i, j, t, k] = a * 16 + b with block row a between i * 2 - 1 and (i + 1) * 2, and block column b equal, modulo 16, to one of j * 2 - 1 to (j + 1) * 2. `counts`: every device's tile (i, j) has some target block with exactly 16 live slots.
All inputs are finite; a program needn't handle non-finite values.
Results may differ from the reference program's by a relative error of at most 0.001.
Values may be sent and summed in bfloat16 or wider, within the bound.
No kernel may reach another device: no remote copies, remote signals or barrier semaphores. Data moves between devices by JAX's collectives and lax.ppermute only.
A program may use at most 192 MiB of HBM per device.

```python
import jax
import jax.numpy as jnp
from jax import lax

BS = 128
BT = 128
SBD = 2
TB = 40
KPT = 16
ROWS = 144
NLB = 32
NOB = 16
N_LAT = 16
N_LON = 8


def draw_source_ids(key, part):
    key_rows, key_cols = jax.random.split(jax.random.fold_in(key, 11))
    shape = (N_LAT, N_LON, TB, KPT)
    lat_grid = jnp.arange(N_LAT, dtype=jnp.int32)[:, None, None, None]
    lon_grid = jnp.arange(N_LON, dtype=jnp.int32)[None, :, None, None]
    lowest = jnp.where(lat_grid == 0, 1, 0)
    highest = jnp.where(lat_grid == N_LAT - 1, SBD, SBD + 1)
    raw_rows = jax.random.randint(key_rows, shape, 0, 1 << 20)
    ext_row = lowest + raw_rows % (highest - lowest + 1)
    ext_col = jax.random.randint(key_cols, shape, 0, SBD + 2)
    cycle_blocks = SBD * N_LON
    block_row = lat_grid * SBD + ext_row - 1
    block_col = (lon_grid * SBD + ext_col - 1 + cycle_blocks) % cycle_blocks
    return (block_row * cycle_blocks + block_col).astype(jnp.int32)


def draw_counts(key, part):
    key_rows, key_cols = jax.random.split(jax.random.fold_in(key, 23))
    drawn = jax.random.randint(key_rows, (N_LAT, N_LON, TB), 0, KPT + 1)
    full_slot = jax.random.randint(key_cols, (N_LAT, N_LON, 1), 0, TB)
    target_index = jnp.arange(TB, dtype=jnp.int32)[None, None, :]
    return jnp.where(target_index == full_slot, KPT, drawn).astype(jnp.int32)


def block_levels(key, extent, cuts, low, largest):
    factor_of = 1.0
    for dim, blocks in cuts:
        steps = jax.random.uniform(jax.random.fold_in(jax.random.fold_in(key, 6), dim), (blocks,), jnp.float32, low / len(cuts), largest / len(cuts))
        factor_of = factor_of * jnp.repeat(jnp.exp(steps), extent[dim] // blocks).reshape((-1,) + (1,) * (len(extent) - 1 - dim))
    return factor_of


def scatter_about(key, extent, width, limit, cuts=(), kind=jnp.bfloat16):
    gain = block_levels(key, extent, cuts, -0.22, 0.18) if cuts else 1.0
    entries = jax.random.normal(key, extent, jnp.float32) * width * gain
    return jnp.minimum(jnp.maximum(entries, -limit), limit).astype(kind)


def setup_inputs(seed: int = 0) -> dict:
    streams_of = jax.random.split(jax.random.key(seed), 6)
    return {
        "increment": scatter_about(streams_of[0], (NLB, NOB, ROWS, BS), 1.0, 6.0, ((0, 16), (1, 8))),
        "cotangent": scatter_about(streams_of[1], (N_LAT, N_LON, TB, ROWS, BT), 1.0, 6.0, ((0, 16), (1, 8))),
        "weights": scatter_about(streams_of[2], (N_LAT, N_LON, TB, KPT, BS, BT), (BS * KPT // 2) ** -0.5, 0.1875, ((0, 16), (1, 8))),
        "source_ids": draw_source_ids(jax.random.fold_in(streams_of[5], 71), 0),
        "counts": draw_counts(jax.random.fold_in(streams_of[5], 71), 0),
    }


def reference(increment, cotangent, weights, source_ids, counts):
    total_blocks = NLB * NOB
    device_count = N_LAT * N_LON
    flattened = increment.reshape(total_blocks, ROWS, BS)
    weight_all = weights.reshape(device_count, TB, KPT, BS, BT)
    source_all = source_ids.reshape(device_count, TB, KPT).astype(jnp.int32)
    count_all = counts.reshape(device_count, TB).astype(jnp.int32)
    cotan_all = cotangent.reshape(device_count, TB, ROWS, BT)

    def device_step(running, pieces):
        weight_dev, source_dev, count_dev, cotan_dev = pieces
        ocean_sum = jnp.zeros((TB, ROWS, BT), jnp.float32)
        cotan_wide = cotan_dev.astype(jnp.float32)
        for slot in range(KPT):
            active = slot < count_dev
            weight_slot = weight_dev[:, slot].astype(jnp.float32)
            picked = flattened[source_dev[:, slot]].astype(jnp.float32) * active.astype(jnp.float32)[:, None, None]
            ocean_sum = ocean_sum + jnp.einsum("tws,tsb->twb", picked, weight_slot)
            contribution = jnp.einsum("twb,tsb->tws", cotan_wide, weight_slot)
            segment = jnp.where(active, source_dev[:, slot], total_blocks).astype(jnp.int32)
            running = running.at[segment].add(contribution)
        return running, ocean_sum.astype(jnp.bfloat16)

    running = jnp.zeros((total_blocks + 1, ROWS, BS), jnp.float32)
    running, ocean = lax.scan(device_step, running, (weight_all, source_all, count_all, cotan_all))
    ocean = ocean.reshape(N_LAT, N_LON, TB, ROWS, BT)
    adjoint_out = running[:total_blocks].reshape(NLB, NOB, ROWS, BS).astype(jnp.bfloat16)
    return ocean, adjoint_out
```

```python
import jax
import jax.numpy as jnp
from jax import lax
from jax.experimental import pallas as pl
from jax.experimental.pallas import tpu as pltpu
from jax.sharding import PartitionSpec as P

W, B, S = 144, 128, 128
TB, KPT = 40, 16
STEP = 2


def ring(value, axis, by):
    n = lax.axis_size(axis)
    return lax.ppermute(value, axis, [(i, (i + by) % n) for i in range(n)])


def line(value, axis, by):
    n = lax.axis_size(axis)
    return lax.ppermute(value, axis, [(i, i + by) for i in range(n) if 0 <= i + by < n])


def adjoint_kernel(pos_ref, cot_ref, w_ref, west, east, north, south, inner, acc):
    step = pl.program_id(0)

    @pl.when(step == 0)
    def _():
        acc[...] = jnp.zeros_like(acc)

    for u in range(STEP):
        t = step * STEP + u
        wt = w_ref[u].reshape(KPT * S, B)
        out = lax.dot_general(
            cot_ref[u], wt, (((1,), (1,)), ((), ())), preferred_element_type=jnp.float32
        )
        for k in range(KPT):
            e = pos_ref[t * KPT + k]
            acc[e] = acc[e] + out[:, k * S:(k + 1) * S]

    @pl.when(step == pl.num_programs(0) - 1)
    def _():
        for r in range(4):
            west[r] = acc[4 * r]
            east[r] = acc[4 * r + 3]
        for c in range(2):
            north[c] = acc[1 + c]
            south[c] = acc[13 + c]
            inner[0, c] = acc[5 + c]
            inner[1, c] = acc[9 + c]


def adjoint(pos, cot, weights):
    block = lambda *s: jax.ShapeDtypeStruct(s + (W, S), jnp.float32)
    whole = lambda *s: pl.BlockSpec(s + (W, S), lambda i, p: (0,) * (len(s) + 2))
    return pl.pallas_call(
        adjoint_kernel,
        grid_spec=pltpu.PrefetchScalarGridSpec(
            num_scalar_prefetch=1,
            grid=(TB // STEP,),
            in_specs=[
                pl.BlockSpec((STEP, W, B), lambda i, p: (i, 0, 0)),
                pl.BlockSpec((STEP, KPT, S, B), lambda i, p: (i, 0, 0, 0)),
            ],
            out_specs=[whole(4), whole(4), whole(2), whole(2), whole(2, 2)],
            scratch_shapes=[pltpu.VMEM((17, W, S), jnp.float32)],
        ),
        out_shape=[block(4), block(4), block(2), block(2), block(2, 2)],
        cost_estimate=pl.CostEstimate(flops=2 * TB * KPT * W * S * B, bytes_accessed=TB * KPT * S * B * 2, transcendentals=0),
        name="adjoint",
    )(pos, cot, weights)


def forward_kernel(pos_ref, own, nb, sb, wb, eb, w_ref, prev, out_ref, ext, sem, *, first):
    step = pl.program_id(0)

    @pl.when(step == 0)
    def _():
        moves = [(wb, slice(0, 4), None)]
        copies = []
        for r in range(4):
            copies.append((wb.at[r], ext.at[4 * r]))
            copies.append((eb.at[r], ext.at[4 * r + 3]))
        for c in range(2):
            copies.append((nb.at[c], ext.at[1 + c]))
            copies.append((sb.at[c], ext.at[13 + c]))
            copies.append((own.at[0, c], ext.at[5 + c]))
            copies.append((own.at[1, c], ext.at[9 + c]))
        for s, d in copies:
            pltpu.make_async_copy(s, d, sem).start()
        ext[16] = jnp.zeros((W, S), jnp.bfloat16)
        for s, d in copies:
            pltpu.make_async_copy(s, d, sem).wait()

    for u in range(STEP):
        t = (step + first) * STEP + u
        lhs = jnp.concatenate([ext[pos_ref[t * KPT + k]] for k in range(KPT)], axis=1)
        wt = w_ref[u].reshape(KPT * S, B)
        out = jnp.dot(lhs, wt, preferred_element_type=jnp.float32)
        out_ref[u] = out.astype(jnp.bfloat16)


def forward(pos, own, nb, sb, wb, eb, weights, prev, first, count):
    import functools
    anyspec = pl.BlockSpec(memory_space=pl.ANY)
    args = [pos, own, nb, sb, wb, eb, weights]
    in_specs = [anyspec] * 5 + [pl.BlockSpec((STEP, KPT, S, B), lambda i, p: (i + first, 0, 0, 0))]
    body = functools.partial(forward_kernel, first=first)
    if prev is None:
        body_fn = lambda p, a, b, c, d, e, w, o, x, s: body(p, a, b, c, d, e, w, None, o, x, s)
        alias = {}
    else:
        body_fn = body
        args.append(prev)
        in_specs.append(anyspec)
        alias = {7: 0}
    return pl.pallas_call(
        body_fn,
        grid_spec=pltpu.PrefetchScalarGridSpec(
            num_scalar_prefetch=1,
            grid=(count,),
            in_specs=in_specs,
            out_specs=pl.BlockSpec((STEP, W, B), lambda i, p: (i + first, 0, 0)),
            scratch_shapes=[pltpu.VMEM((17, W, S), jnp.bfloat16), pltpu.SemaphoreType.DMA],
        ),
        out_shape=jax.ShapeDtypeStruct((TB, W, B), jnp.bfloat16),
        input_output_aliases=alias,
        cost_estimate=pl.CostEstimate(flops=2 * count * STEP * KPT * W * S * B, bytes_accessed=count * STEP * KPT * S * B * 2, transcendentals=0),
        name="forward",
    )(*args)


def body(increment, cotangent, weights, source_ids, counts):
    side = increment.shape[0]
    cols = side * lax.axis_size("lon")
    ids = source_ids[0, 0]
    row = ids // cols - lax.axis_index("lat") * side + 1
    col = (ids % cols - lax.axis_index("lon") * side + 1 + cols) % cols
    live = jnp.arange(KPT, dtype=jnp.int32)[None, :] < counts[0, 0][:, None]
    pos = jnp.where(live, row * 4 + col, 16).astype(jnp.int32).reshape(-1)
    w = weights[0, 0]

    nb = line(increment[1:2], "lat", 1)[0]
    sb = line(increment[0:1], "lat", -1)[0]
    column = lambda c: jnp.concatenate([nb[c][None], increment[:, c], sb[c][None]])
    wb = ring(column(1), "lon", 1)
    eb = ring(column(0), "lon", -1)

    west, east, north, south, inner = adjoint(pos, cotangent[0, 0], w)
    fw = ring(east, "lon", 1)
    fe = ring(west, "lon", -1)
    ocean = forward(pos, increment, nb, sb, wb, eb, w, None, 0, 8)
    lon_in = jnp.stack([fw, fe], axis=1)
    fn = line(south + lon_in[3], "lat", 1)
    fs = line(north + lon_in[0], "lat", -1)
    ocean = forward(pos, increment, nb, sb, wb, eb, w, ocean, 8, 12)
    total = inner + lon_in[1:3] + jnp.stack([fn, fs])
    return ocean[None, None], total.astype(jnp.bfloat16)


def solution(mesh):
    placed = (
        P("lat", "lon", None, None),
        P("lat", "lon", None, None, None),
        P("lat", "lon", None, None, None, None),
        P("lat", "lon", None, None),
        P("lat", "lon", None),
    )
    return jax.shard_map(
        body,
        mesh=mesh,
        in_specs=placed,
        out_specs=(P("lat", "lon", None, None, None), P("lat", "lon", None, None)),
        check_vma=False,
    )
```

```python
import functools
import jax
import jax.numpy as jnp
from jax import lax
from jax.experimental import pallas as pl
from jax.experimental.pallas import tpu as pltpu
from jax.sharding import PartitionSpec as P

W, B, S = 144, 128, 128
TB, KPT = 40, 16
G = 4
CH = KPT // G
NBLK = TB * CH
UN = 8
NACC = 4
LAG = 3
WAIT_AT = UN - 2
FRONT = 4


def slot_place(ids, counts, lat2, lon2, t, k):
    s = ids[t, k]
    e = ((s >> 4) - lat2 + 1) * 4 + ((s - lon2 + 1) & 15)
    return jnp.where(k < counts[t], e, 16)


def start_copies(counts, w, lst, wbuf, sems):
    def start(v, b):
        pltpu.make_async_copy(w.at[v], wbuf.at[b], sems.at[b >> 3]).start()

    for i in range(FRONT):
        lst[i] = NBLK
    pos = jnp.int32(0)
    for t in range(TB):
        n = counts[t]
        for q in range(CH):
            if w is not None:
                @pl.when(n > q * G)
                def _(v=t * CH + q, b=pos + q):
                    start(v, b)
            lst[pos + (FRONT + q)] = t * CH + q
        pos = pos + ((n + (G - 1)) >> 2)
    trips = (pos + (UN - 1)) >> 3
    for q in range(UN + 1):
        lst[pos + (FRONT + q)] = NBLK
    for q in range(UN - 1 if w is not None else 0):
        @pl.when(pos + q < trips * UN)
        def _(b=pos + q):
            start(0, b)
    return trips


def run_blocks(trips, w, lst, wbuf, sems, accs, setup, lhs_of, tile_of, emit):
    total = trips * UN
    setup()

    def await_trip(i):
        if w is None:
            return

        @pl.when(i < trips)
        def _():
            pltpu.make_async_copy(
                w.at[pl.ds(0, UN)], wbuf.at[pl.ds(i * UN, UN)], sems.at[i]
            ).wait()

    for q in range(2):
        for u in range(NACC):
            pltpu.matmul_pop(accs[q][u])
    await_trip(0)
    for q in range(2):
        pltpu.matmul_push_rhs(tile_of(wbuf, 0, q), staging_register=0, mxu_index=q)

    def trip(i, _):
        b0 = i * UN
        for u in range(UN):
            b = b0 + u
            v = lst[b + FRONT]
            for q in range(2):
                pltpu.matmul_acc_lhs(accs[q][u % NACC], lhs_of(v, q), load_staged_rhs=u % 2)
            if u == WAIT_AT:
                await_trip(i + 1)
            for q in range(2):
                pltpu.matmul_push_rhs(tile_of(wbuf, b + 1, q), staging_register=(u + 1) % 2, mxu_index=q)
            done = lst[b + FRONT - LAG]
            emit(done, [pltpu.matmul_pop(accs[q][(u + 1) % NACC]) for q in range(2)])
        return 0

    lax.fori_loop(0, trips, trip, 0)
    zero = jnp.zeros((W, 256), jnp.bfloat16)
    for q in range(2):
        pltpu.matmul_acc_lhs(accs[q][0], zero, load_staged_rhs=0)
    for u in range(1, NACC):
        done = lst[total + FRONT - (NACC - u)]
        emit(done, [pltpu.matmul_pop(accs[q][u]) for q in range(2)])
    for q in range(2):
        pltpu.matmul_pop(accs[q][0])


def acc_refs():
    return [[pltpu.ACC(q)((W, 256), jnp.float32) for _ in range(NACC)] for q in range(2)]


def adjoint_kernel(ids, counts, cot, w, west, east, north, south, inner, wbuf, acc, lst, sems):
    lat2 = lax.axis_index("lat") * 2
    lon2 = lax.axis_index("lon") * 2

    def run(*flat):
        accs = [flat[:NACC], flat[NACC:]]

        def setup():
            acc[...] = jnp.zeros_like(acc)

        def lhs_of(v, q):
            t = jnp.minimum(v >> 2, TB - 1)
            return jnp.concatenate([cot[t], jnp.zeros((W, B), jnp.bfloat16)], axis=1)

        def tile_of(buf, b, q):
            pair = buf[b, pl.ds(2 * q, 2)].reshape(2 * S, B).T
            return jnp.concatenate([pair, jnp.zeros((B, 2 * S), jnp.bfloat16)], axis=0)

        def emit(v, pops):
            t = jnp.minimum(v >> 2, TB - 1)
            base = (v & 3) * G
            dead = v >= NBLK
            for q in range(2):
                for h in range(2):
                    k = base + 2 * q + h
                    e = slot_place(ids, counts, lat2, lon2, t, k)
                    e = jnp.where(dead, 16, e)
                    acc[e] = acc[e] + pops[q][:, h * S:(h + 1) * S]

        run_blocks(start_copies(counts, w, lst, wbuf, sems), w, lst, wbuf, sems, accs, setup, lhs_of, tile_of, emit)

    pl.run_scoped(run, *[a for q in acc_refs() for a in q])
    for r in range(4):
        west[r] = acc[4 * r]
        east[r] = acc[4 * r + 3]
    for c in range(2):
        north[c] = acc[1 + c]
        south[c] = acc[13 + c]
        inner[0, c] = acc[5 + c]
        inner[1, c] = acc[9 + c]


VM = pl.BlockSpec(memory_space=pltpu.VMEM)
SM = pl.BlockSpec(memory_space=pltpu.SMEM)
HB = pl.BlockSpec(memory_space=pl.ANY)


LIMIT = 14 << 20
WBUF = pltpu.VMEM((NBLK + 1, G, S, B), jnp.bfloat16)


def scratch():
    return [
        pltpu.SMEM((NBLK + 2 * UN + 2 * FRONT,), jnp.int32),
        pltpu.SemaphoreType.DMA((NBLK // UN,)),
    ]


def adjoint(ids, counts, cot, weights):
    block = lambda *s: jax.ShapeDtypeStruct(s + (W, S), jnp.float32)
    return pl.pallas_call(
        adjoint_kernel,
        in_specs=[SM, SM, VM, HB],
        out_specs=[VM] * 6,
        scratch_shapes=[pltpu.VMEM((17, W, S), jnp.float32)] + scratch(),
        out_shape=[block(4), block(4), block(2), block(2), block(2, 2), WBUF],
        compiler_params=pltpu.CompilerParams(vmem_limit_bytes=LIMIT),
        cost_estimate=pl.CostEstimate(flops=2 * TB * KPT * W * S * B, bytes_accessed=TB * KPT * S * B * 2, transcendentals=0),
        name="adjoint",
    )(ids, counts, cot, weights.reshape(NBLK, G, S, B))


def forward_kernel(ids, counts, own, nb, sb, wb, eb, wbuf, out, sums, ext, sem, lst, sems):
    lat2 = lax.axis_index("lat") * 2
    lon2 = lax.axis_index("lon") * 2
    copies = []
    for r in range(4):
        copies.append((wb.at[r], ext.at[4 * r]))
        copies.append((eb.at[r], ext.at[4 * r + 3]))
    for c in range(2):
        copies.append((nb.at[c], ext.at[1 + c]))
        copies.append((sb.at[c], ext.at[13 + c]))
        copies.append((own.at[0, c], ext.at[5 + c]))
        copies.append((own.at[1, c], ext.at[9 + c]))
    copies = [pltpu.make_async_copy(s, d, sem.at[i]) for i, (s, d) in enumerate(copies)]

    def run(*flat):
        accs = [flat[:NACC], flat[NACC:]]

        def setup():
            for c in copies:
                c.start()
            sums[...] = jnp.zeros_like(sums)
            ext[16] = jnp.zeros((W, S), jnp.bfloat16)
            for c in copies:
                c.wait()

        def lhs_of(v, q):
            t = jnp.minimum(v >> 2, TB - 1)
            base = (v & 3) * G
            dead = v >= NBLK
            parts = []
            for h in range(2):
                e = slot_place(ids, counts, lat2, lon2, t, base + 2 * q + h)
                parts.append(ext[jnp.where(dead, 16, e)])
            return jnp.concatenate(parts, axis=1)

        def tile_of(buf, b, q):
            pair = buf[b, pl.ds(2 * q, 2)].reshape(2 * S, B)
            return jnp.concatenate([pair, jnp.zeros((2 * S, B), jnp.bfloat16)], axis=1)

        def emit(v, pops):
            t = v >> 2
            sums[t] = sums[t] + (pops[0][:, :B] + pops[1][:, :B])

        run_blocks(start_copies(counts, None, lst, wbuf, None), None, lst, wbuf, None, accs, setup, lhs_of, tile_of, emit)

    pl.run_scoped(run, *[a for q in acc_refs() for a in q])

    def finish(t, _):
        out[t] = sums[t].astype(jnp.bfloat16)
        return 0

    lax.fori_loop(0, TB, finish, 0, unroll=2)


def forward(ids, counts, own, nb, sb, wb, eb, wbuf):
    return pl.pallas_call(
        forward_kernel,
        in_specs=[SM, SM] + [HB] * 5 + [VM],
        out_specs=VM,
        scratch_shapes=[
            pltpu.VMEM((TB + 1, W, B), jnp.float32),
            pltpu.VMEM((17, W, S), jnp.bfloat16),
            pltpu.SemaphoreType.DMA((16,)),
        ] + scratch(),
        out_shape=jax.ShapeDtypeStruct((TB, W, B), jnp.bfloat16),
        compiler_params=pltpu.CompilerParams(vmem_limit_bytes=LIMIT),
        cost_estimate=pl.CostEstimate(flops=2 * TB * KPT * W * S * B, bytes_accessed=TB * KPT * S * B * 2, transcendentals=0),
        name="forward",
    )(ids, counts, own, nb, sb, wb, eb, wbuf)


def ring(value, axis, by):
    n = lax.axis_size(axis)
    return lax.ppermute(value, axis, [(i, (i + by) % n) for i in range(n)])


def line(value, axis, by):
    n = lax.axis_size(axis)
    return lax.ppermute(value, axis, [(i, i + by) for i in range(n) if 0 <= i + by < n])


def body(increment, cotangent, weights, source_ids, counts):
    ids, live, w = source_ids[0, 0], counts[0, 0], weights[0, 0]
    nb = line(increment[1:2], "lat", 1)[0]
    sb = line(increment[0:1], "lat", -1)[0]
    column = lambda c: jnp.concatenate([nb[c][None], increment[:, c], sb[c][None]])
    wb = ring(column(1), "lon", 1)
    eb = ring(column(0), "lon", -1)
    west, east, north, south, inner, wbuf = adjoint(ids, live, cotangent[0, 0], w)
    fw = ring(east, "lon", 1)
    fe = ring(west, "lon", -1)
    lon_in = jnp.stack([fw, fe], axis=1)
    fn = line(south + lon_in[3], "lat", 1)
    fs = line(north + lon_in[0], "lat", -1)
    ocean = forward(ids, live, increment, nb, sb, wb, eb, wbuf)
    total = inner + lon_in[1:3] + jnp.stack([fn, fs])
    return ocean[None, None], total.astype(jnp.bfloat16)


def solution(mesh):
    placed = (
        P("lat", "lon", None, None),
        P("lat", "lon", None, None, None),
        P("lat", "lon", None, None, None, None),
        P("lat", "lon", None, None),
        P("lat", "lon", None),
    )
    return jax.shard_map(
        body,
        mesh=mesh,
        in_specs=placed,
        out_specs=(P("lat", "lon", None, None, None), P("lat", "lon", None, None)),
        check_vma=False,
    )
```
